32 devices in a mesh: dp: 8 (over z, core), tensor: 4 (over y, x).
Axes of the slice: x: 2, y: 2, z: 4, core: 2. Of those that a mesh axis runs over, the one named last changes fastest.
Arguments:
- token_ids: int32 [8, 1024], P('dp', 'tensor'), may hold values from 0 to 30527
- lengths: int32 [8], P('dp'), may hold values from 256 to 1024, as said below
- teacher_bins: int32 [8], P('dp'), may hold values from 0 to 127
- embed_table: bfloat16 [30528, 1024], P('tensor'), may hold values from -6 to 6
- query_key_value_matrix: bfloat16 [1024, 3, 1024], P('dp', None, 'tensor'), may hold values from -2 to 2
- output_matrix: bfloat16 [1024, 1024], P('tensor', 'dp'), may hold values from -0.1875 to 0.1875
- up_matrix: bfloat16 [1024, 4096], P('dp', 'tensor'), may hold values from -0.1875 to 0.1875
- down_matrix: bfloat16 [4096, 1024], P('tensor', 'dp'), may hold values from -0.09375 to 0.09375
- w_head: bfloat16 [1024, 128], P('dp'), may hold values from -64 to 64
Outputs:
- loss: float32 [], replicated
- query_key_value_gradient: float32 [1024, 3, 1024], P('dp', None, 'tensor')
- output_weight_gradient: float32 [1024, 1024], P('tensor', 'dp')
- up_weight_gradient: float32 [1024, 4096], P('dp', 'tensor')
- down_weight_gradient: float32 [4096, 1024], P('tensor', 'dp')
- grad_head: float32 [1024, 128], P('dp')
The draws below stay inside these ranges and needn't reach their ends.
Inputs may be any that keep to these rules, and one draw needn't show every extreme that they name: lengths[0] is 1024.
All inputs are finite; a program needn't handle non-finite values.
Results may differ from the reference program's by a relative error of at most 0.02.
Values may be sent and summed in bfloat16 or wider, within the bound.
No kernel may reach another device: no remote copies, remote signals or barrier semaphores. Data moves between devices by JAX's collectives and lax.ppermute only.
A program may use at most 128 MiB of HBM per device.

```python
import math
import jax
import jax.numpy as jnp
import numpy as np
from jax import lax

D = 1024
HEAD_COUNT = 16
HEAD_WIDTH = 64
FF = 4096
VOCAB = 30528
NBINS = 128
LEN = 1024
SEQS = 8
N_TENSOR = 4


def draw_lengths(key, part):
    values = jax.random.randint(jax.random.fold_in(key, 11), (SEQS,), LEN // 4, LEN + 1, dtype=jnp.int32)
    return values.at[0].set(LEN)


def draw_embed_table(key, part):
    normal_rows = jax.random.normal(jax.random.fold_in(key, 21), (VOCAB, D), jnp.float32)
    values = normal_rows
    return jnp.clip(values, -6.0, 6.0).astype(jnp.bfloat16)


def draw_query_key_value_matrix(key, part):
    scaled = jnp.clip(jax.random.normal(jax.random.fold_in(key, 31), (D, 3, D), jnp.float32), -6.0, 6.0) * (1.0 / math.sqrt(D))
    return jnp.clip(scaled, -2.0, 2.0).astype(jnp.bfloat16)


def draw_w_head(key, part):
    drawn_cols = jnp.clip(jax.random.normal(jax.random.fold_in(key, 41), (D, NBINS), jnp.float32), -6.0, 6.0) * 0.1
    return jnp.clip(drawn_cols, -64.0, 64.0).astype(jnp.bfloat16)


def plant(entries, rng, least, top_value):
    longest = entries.shape.index(max(entries.shape))
    spots = []
    for shift in (0, 1):
        where = [jax.random.randint(jax.random.fold_in(rng, axis), (), 0, length) for axis, length in enumerate(entries.shape)]
        where[longest] = (where[longest] + shift) % entries.shape[longest]
        spots.append(tuple(where))
    return entries.at[spots[0]].set(least).at[spots[1]].set(top_value)


def shard_levels(own_key, extent, cuts, smallest, high):
    def one(axis_at, parts):
        heights = jax.random.uniform(jax.random.fold_in(jax.random.fold_in(own_key, 6), axis_at), (parts,), jnp.float32, smallest / len(cuts), high / len(cuts))
        return jnp.repeat(jnp.exp(heights), extent[axis_at] // parts).reshape((-1,) + (1,) * (len(extent) - axis_at - 1))

    loudness = one(*cuts[0])
    for cut in cuts[1:]:
        loudness = loudness * one(*cut)
    return loudness


def rank_table(amount, slope):
    portions = [(1 << 20) // math.isqrt(standing ** slope) + 1 for standing in range(1, amount + 1)]
    scale = 1 + sum(portions) // (1 << 30)
    return np.cumsum(np.array([max(1, weight // scale) for weight in portions]))


def skewed_ids(stream_key, extent, amount, lean):
    listing = rank_table(amount, lean)
    ticket = jax.random.randint(jax.random.fold_in(stream_key, 1), extent, 0, int(listing[amount - 1]))
    rank = jnp.searchsorted(jnp.asarray(listing, jnp.int32), ticket, side="right")
    return jax.random.permutation(jax.random.fold_in(stream_key, 2), amount)[rank].astype(jnp.int32)


def normal_values(key, shape, scale, reach, shards=(), held_as=jnp.bfloat16):
    values = jax.random.normal(key, shape, jnp.float32) * scale
    if len(shards) > 0:
        values = shard_levels(key, shape, shards, -0.22, 0.18) * values
    return jnp.clip(values, min=-reach, max=reach).astype(held_as)


def setup_inputs(seed: int = 0) -> dict:
    streams_of = jax.random.split(jax.random.key(seed), 10)
    token_ids = plant(skewed_ids(streams_of[0], (SEQS, LEN), VOCAB, 2), jax.random.fold_in(streams_of[0], 3), 0, VOCAB - 1).astype(jnp.int32)
    lengths = draw_lengths(jax.random.fold_in(streams_of[9], 71), 0)
    teacher_bins = plant(jax.random.randint(streams_of[2], (SEQS,), 0, NBINS), jax.random.fold_in(streams_of[2], 1), 0, NBINS - 1).astype(jnp.int32)
    embed_table = draw_embed_table(jax.random.fold_in(streams_of[9], 71), 0)
    query_key_value_matrix = draw_query_key_value_matrix(jax.random.fold_in(streams_of[9], 71), 0)
    output_matrix = normal_values(streams_of[5], (D, D), D ** -0.5, 0.1875, ((0, 4), (1, 8)))
    up_matrix = normal_values(streams_of[6], (D, FF), D ** -0.5, 0.1875, ((0, 8), (1, 4)))
    down_matrix = normal_values(streams_of[7], (FF, D), FF ** -0.5, 0.09375, ((0, 4), (1, 8)))
    w_head = draw_w_head(jax.random.fold_in(streams_of[9], 71), 0)
    return dict(token_ids=token_ids, lengths=lengths, teacher_bins=teacher_bins, embed_table=embed_table, query_key_value_matrix=query_key_value_matrix, output_matrix=output_matrix, up_matrix=up_matrix, down_matrix=down_matrix, w_head=w_head)


EPS = 1e-05

def normalize(values):
    mean = lax.optimization_barrier(jnp.mean(values, axis=-1, keepdims=True))
    centered = values - mean
    return centered * lax.rsqrt(lax.optimization_barrier(jnp.mean(centered * centered, axis=-1, keepdims=True)) + EPS)

def gelu_tanh(values):
    return 0.5 * values * (1.0 + jnp.tanh(0.7978845608028654 * (values + 0.044715 * values * values * values)))

def attend(query, keys, values_in, lengths):
    scale = query.shape[-1] ** (-0.5)
    scores = jnp.einsum('sqhe,skhe->shqk', query, keys) * scale
    visible = jnp.arange(keys.shape[1], dtype=jnp.int32)[None, :] < lengths[:, None]
    scores = jnp.where(visible[:, None, None, :], scores, -1e+30)
    top = lax.optimization_barrier(jnp.max(scores, axis=-1, keepdims=True))
    expo = jnp.exp(scores - top)
    probs = expo / lax.optimization_barrier(jnp.sum(expo, axis=-1, keepdims=True))
    rounded = lax.optimization_barrier(probs.astype(jnp.bfloat16)).astype(jnp.float32)
    return jnp.einsum('shqk,skhe->sqhe', rounded, values_in)

def rounded_sum(left_operand, right_operand, blocks, inner_value):
    total = None
    for layer_block in range(blocks):
        slice_portion = jnp.einsum('wou,ue->woe', left_operand[:, :, layer_block * inner_value:(layer_block + 1) * inner_value].astype(jnp.float32), right_operand[layer_block * inner_value:(layer_block + 1) * inner_value].astype(jnp.float32))
        slice_portion = lax.optimization_barrier(slice_portion.astype(jnp.bfloat16)).astype(jnp.float32)
        total = slice_portion if total is None else total + slice_portion
    return total

def reference(token_ids, lengths, teacher_bins, embed_table, query_key_value_matrix, output_matrix, up_matrix, down_matrix, w_head):
    sequence_batch, sequence_length = token_ids.shape
    width = embed_table.shape[1]
    first = jnp.take(embed_table, token_ids, axis=0)
    first_normed_rows = normalize(first.astype(jnp.float32)).astype(jnp.bfloat16)
    mixed_output = jnp.einsum('fxw,wvr->fxvr', first_normed_rows.astype(jnp.float32), query_key_value_matrix.astype(jnp.float32)).astype(jnp.bfloat16)
    split = mixed_output.astype(jnp.float32).reshape(sequence_batch, sequence_length, 3, HEAD_COUNT, HEAD_WIDTH)

    def forward_one(item):
        query, keys, vals, count = item
        return attend(query[None], keys[None], vals[None], count[None])[0]
    attended_rows = lax.map(forward_one, (split[:, :, 0], split[:, :, 1], split[:, :, 2], lengths))
    attended_rows = attended_rows.astype(jnp.bfloat16).reshape(sequence_batch, sequence_length, width)
    attn = rounded_sum(attended_rows, output_matrix, N_TENSOR, width // N_TENSOR)
    second = (first.astype(jnp.float32) + attn).astype(jnp.bfloat16)
    second_normed_rows = normalize(second.astype(jnp.float32)).astype(jnp.bfloat16)
    hidden_preactivation = jnp.einsum('ntp,pk->ntk', second_normed_rows.astype(jnp.float32), up_matrix.astype(jnp.float32))
    hidden_activated = gelu_tanh(hidden_preactivation).astype(jnp.bfloat16)
    ffn = rounded_sum(hidden_activated, down_matrix, N_TENSOR, FF // N_TENSOR)
    third = second.astype(jnp.float32) + ffn
    live = (jnp.arange(sequence_length, dtype=jnp.int32)[None, :] < lengths[:, None]).astype(jnp.float32)
    counts = lengths.astype(jnp.float32)[:, None]
    pooled = lax.optimization_barrier(jnp.sum(third * live[:, :, None], axis=1)) / counts
    final, final_back = jax.vjp(normalize, pooled)
    head = w_head.astype(jnp.float32)
    logits = jnp.dot(final, head, precision=lax.Precision.HIGHEST)
    top = lax.optimization_barrier(jnp.max(logits, axis=-1, keepdims=True))
    total_exp = jnp.log(lax.optimization_barrier(jnp.sum(jnp.exp(logits - top), axis=-1, keepdims=True))) + top
    labels = (teacher_bins[:, None] == jnp.arange(logits.shape[1], dtype=jnp.int32)[None, :]).astype(jnp.float32)
    losses = total_exp[:, 0] - lax.optimization_barrier(jnp.sum(logits * labels, axis=-1))
    loss = jnp.sum(losses) / sequence_batch
    g_logits = (jnp.exp(logits - total_exp) - labels) / sequence_batch
    grad_head = jnp.dot(final.T, g_logits, precision=lax.Precision.HIGHEST)
    g_final = jnp.dot(g_logits, head.T, precision=lax.Precision.HIGHEST)
    g_pooled = final_back(g_final)[0]
    per_token = g_pooled / counts
    g_third = per_token[:, None, :] * live[:, :, None]
    third_gradient_batch = g_third.astype(jnp.bfloat16)
    down_weight_gradient = jnp.einsum('omi,omy->iy', hidden_activated.astype(jnp.float32), third_gradient_batch.astype(jnp.float32))
    hidden_gradient = jnp.einsum('tpu,bu->tpb', third_gradient_batch.astype(jnp.float32), down_matrix.astype(jnp.float32))
    gelu_back = jax.vjp(gelu_tanh, hidden_preactivation)[1]
    preact_gradient = gelu_back(hidden_gradient)[0].astype(jnp.bfloat16)
    up_weight_gradient = jnp.einsum('qon,qom->nm', second_normed_rows.astype(jnp.float32), preact_gradient.astype(jnp.float32))
    g_normed_two = rounded_sum(preact_gradient, up_matrix.T, N_TENSOR, FF // N_TENSOR)
    norm_back = jax.vjp(normalize, second.astype(jnp.float32))[1]
    second_gradient = (g_third + norm_back(g_normed_two)[0]).astype(jnp.bfloat16)
    output_weight_gradient = jnp.einsum('jxm,jxn->mn', attended_rows.astype(jnp.float32), second_gradient.astype(jnp.float32))
    attended_gradient = jnp.einsum('kmi,qi->kmq', second_gradient.astype(jnp.float32), output_matrix.astype(jnp.float32)).reshape(sequence_batch, sequence_length, HEAD_COUNT, HEAD_WIDTH)

    def backward_one(item):
        query, keys, vals, count, grad = item
        back = jax.vjp(lambda a, b, c: attend(a[None], b[None], c[None], count[None])[0], query, keys, vals)[1]
        return back(grad)
    g_query, g_keys, g_vals = lax.map(backward_one, (split[:, :, 0], split[:, :, 1], split[:, :, 2], lengths, attended_gradient))
    mixed_gradient = jnp.stack([g_query, g_keys, g_vals], axis=2).reshape(sequence_batch, sequence_length, 3, width).astype(jnp.bfloat16)
    query_key_value_gradient = jnp.einsum('rvt,rvzx->tzx', first_normed_rows.astype(jnp.float32), mixed_gradient.astype(jnp.float32))
    return (loss, query_key_value_gradient, output_weight_gradient, up_weight_gradient, down_weight_gradient, grad_head)
```

```python
import jax
import jax.numpy as jnp
from jax import lax
from jax.sharding import PartitionSpec as P

HEAD_WIDTH = 64
EPS = 1e-05
GELU_C = 0.7978845608028654
GELU_A = 0.044715


F32 = jnp.float32
BF16 = jnp.bfloat16


def normalize(values):
    mean = jnp.mean(values, axis=-1, keepdims=True)
    centered = values - mean
    return centered * lax.rsqrt(jnp.mean(centered * centered, axis=-1, keepdims=True) + EPS)


def gelu_and_slope(v):
    inner = GELU_C * (v + GELU_A * v * v * v)
    t = jnp.tanh(inner)
    act = 0.5 * v * (1.0 + t)
    slope = 0.5 * (1.0 + t) + 0.5 * v * (1.0 - t * t) * GELU_C * (1.0 + 3.0 * GELU_A * v * v)
    return act, slope


def mm(a, b, spec):
    return jnp.einsum(spec, a, b, preferred_element_type=F32)


class Tensor:
    def __init__(self):
        self.n = lax.axis_size("tensor")
        self.rank = lax.axis_index("tensor")
        self.xor = self.n & (self.n - 1) == 0

    def to(self, r, j):
        return r ^ j if self.xor else (r + j) % self.n

    def send(self, value, j):
        return lax.ppermute(value, "tensor", [(r, self.to(r, j)) for r in range(self.n)])

    def fetch(self, value, j):
        return lax.ppermute(value, "tensor", [(self.to(r, j), r) for r in range(self.n)])

    def gather(self, value):
        return [value] + [self.fetch(value, j) for j in range(1, self.n)]


class Groups:
    def __init__(self):
        self.n = lax.axis_size("dp")
        self.w = 2 if self.n % 2 == 0 else 1
        self.m = self.n // self.w
        idx = lax.axis_index("dp")
        self.idx = idx
        self.z = idx // self.w
        self.c = idx % self.w

    def shift(self, value, k):
        pairs = []
        for z in range(self.m):
            for c in range(self.w):
                pairs.append((((z + k) % self.m) * self.w + c, z * self.w + c))
        return lax.ppermute(value, "dp", pairs)

    def swap(self, value):
        pairs = [(i, i ^ 1) for i in range(self.n)]
        return lax.ppermute(value, "dp", pairs)

    def gather(self, shard):
        parts = [shard] + [self.shift(shard, k) for k in range(1, self.m)]
        twice = jnp.stack(parts + parts[:-1], axis=0)
        ordered = lax.dynamic_slice_in_dim(twice, (self.m - self.z) % self.m, self.m, axis=0)
        if self.w == 1:
            return ordered
        other = self.swap(ordered)
        low = jnp.where(self.c == 0, ordered, other)
        high = jnp.where(self.c == 0, other, ordered)
        return jnp.stack([low, high], axis=1).reshape((self.n,) + shard.shape)

    def reduce(self, blocks):
        t = blocks.reshape((self.m, self.w) + blocks.shape[1:])
        if self.w == 2:
            away = jnp.where(self.c == 0, t[:, 1], t[:, 0])
            keep = jnp.where(self.c == 0, t[:, 0], t[:, 1])
            pair = (keep.astype(F32) + self.swap(away).astype(F32)).astype(BF16)
        else:
            pair = t[:, 0]
        total = lax.dynamic_index_in_dim(pair, self.z, 0, keepdims=False).astype(F32)
        for k in range(1, self.m):
            out = lax.dynamic_index_in_dim(pair, (self.z + self.m - k) % self.m, 0, keepdims=False)
            total = total + self.shift(out, k).astype(F32)
        return total


def rows_full(blocks):
    return blocks.reshape((blocks.shape[0] * blocks.shape[1],) + blocks.shape[2:])


def cols_full(blocks):
    return jnp.moveaxis(blocks, 0, 1).reshape(blocks.shape[1], -1)


def per_device(
    token_ids,
    lengths,
    teacher_bins,
    embed_table,
    query_key_value_matrix,
    output_matrix,
    up_matrix,
    down_matrix,
    w_head,
):
    tp = Tensor()
    dp = Groups()
    nt = tp.n
    groups, local_len = token_ids.shape
    total_len = local_len * nt
    width = embed_table.shape[1]
    vocab_local = embed_table.shape[0]
    blocks = range(nt)

    ids = tp.gather(token_ids)

    def rows_for(j):
        shifted = ids[j] - tp.rank * vocab_local
        inside = (shifted >= 0) & (shifted < vocab_local)
        rows = jnp.take(embed_table, jnp.clip(shifted, 0, vocab_local - 1), axis=0)
        return jnp.where(inside[..., None], rows, jnp.zeros((), BF16))

    order = list(range(1, nt))[::-1]
    arrived = [tp.send(rows_for(j), j) for j in order]
    first_f = rows_for(0).astype(F32)
    for piece in arrived:
        first_f = first_f + piece.astype(F32)
    first_normed = normalize(first_f).astype(BF16)
    normed = tp.gather(first_normed)

    qkv_w = rows_full(dp.gather(query_key_value_matrix.reshape(query_key_value_matrix.shape[0], -1)))
    out_w = cols_full(dp.gather(output_matrix))
    up_w = rows_full(dp.gather(up_matrix))
    down_w = cols_full(dp.gather(down_matrix))
    head_w = rows_full(dp.gather(w_head)).astype(F32)

    cols = query_key_value_matrix.shape[2]
    heads = cols // HEAD_WIDTH
    qkv = jnp.concatenate(
        [mm(normed[j], qkv_w, "nld,dc->nlc").astype(BF16) for j in blocks], axis=1
    )
    split = qkv.reshape(groups, total_len, 3, heads, HEAD_WIDTH)
    query, keys, vals = split[:, :, 0], split[:, :, 1], split[:, :, 2]

    at = [tp.to(tp.rank, j) * local_len + jnp.arange(local_len, dtype=jnp.int32) for j in blocks]
    live = [(at[j][None, :] < lengths[:, None]).astype(F32) for j in blocks]
    live_all = jnp.concatenate(live, axis=1)
    scale = HEAD_WIDTH ** (-0.5)

    probs = [None] * nt
    context = [None] * nt
    arrived = []
    for j in order + [0]:
        q = query[:, j * local_len : (j + 1) * local_len]
        scores = mm(q, keys, "nqhe,nkhe->nhqk") * scale
        scores = jnp.where(live_all[:, None, None, :] > 0, scores, -1e30)
        top = jnp.max(scores, axis=-1, keepdims=True)
        expo = jnp.exp(scores - top)
        probs[j] = (expo / jnp.sum(expo, axis=-1, keepdims=True)).astype(BF16)
        got = mm(probs[j], vals, "nhqk,nkhe->nqhe").astype(BF16)
        context[j] = got.reshape(groups, local_len, cols)
        part = mm(context[j], out_w, "nlh,hd->nld").astype(BF16)
        if j:
            arrived.append(tp.send(part, j))
        else:
            attn_sum = part.astype(F32)
    for piece in arrived:
        attn_sum = attn_sum + piece.astype(F32)
    second = (first_f + attn_sum).astype(BF16)
    second_f = second.astype(F32)
    normed_two_f, norm_back = jax.vjp(normalize, second_f)
    normed_two = tp.gather(normed_two_f.astype(BF16))

    slopes = []
    hidden_sum = 0.0
    for j in blocks:
        act, slope = gelu_and_slope(mm(normed_two[j], up_w, "nld,df->nlf"))
        slopes.append((slope * live[j][:, :, None]).astype(BF16))
        hidden_sum = hidden_sum + jnp.sum(
            act.astype(BF16).astype(F32) * live[j][:, :, None], axis=1
        )
    coarse = hidden_sum.astype(BF16)
    fine = (hidden_sum - coarse.astype(F32)).astype(BF16)
    pooled_part = mm(jnp.stack([coarse, fine]), down_w, "knf,fd->knd").sum(axis=0)
    pooled_part = pooled_part + jnp.sum(second_f * live[0][:, :, None], axis=1)
    counts = lengths.astype(F32)[:, None]
    pooled_sum = pooled_part
    for piece in tp.gather(pooled_part)[1:]:
        pooled_sum = pooled_sum + piece
    pooled = pooled_sum / counts
    final, final_back = jax.vjp(normalize, pooled)
    logits = jnp.dot(final, head_w, precision=lax.Precision.HIGHEST)
    top = jnp.max(logits, axis=-1, keepdims=True)
    total_exp = jnp.log(jnp.sum(jnp.exp(logits - top), axis=-1, keepdims=True)) + top
    labels = (
        teacher_bins[:, None] == jnp.arange(logits.shape[1], dtype=jnp.int32)[None, :]
    ).astype(F32)
    losses = total_exp[:, 0] - jnp.sum(logits * labels, axis=-1)
    total_seqs = groups * dp.n
    g_logits = (jnp.exp(logits - total_exp) - labels) / total_seqs
    g_final = jnp.dot(g_logits, head_w.T, precision=lax.Precision.HIGHEST)
    g_pooled = final_back(g_final)[0]
    per_token = g_pooled / counts
    per_token_b = per_token.astype(BF16)

    hidden_g = mm(per_token_b, down_w, "nd,fd->nf")
    g_pre = [(slopes[j].astype(F32) * hidden_g[:, None, :]).astype(BF16) for j in blocks]
    arrived = []
    for j in order:
        part = mm(g_pre[j], up_w, "nlf,df->nld").astype(BF16)
        arrived.append(tp.send(part, j))
    g_normed_two = mm(g_pre[0], up_w, "nlf,df->nld").astype(BF16).astype(F32)
    for piece in arrived:
        g_normed_two = g_normed_two + piece.astype(F32)
    g_third = per_token[:, None, :] * live[0][:, :, None]
    g_second = tp.gather((g_third + norm_back(g_normed_two)[0]).astype(BF16))

    sizes = (hidden_sum.shape[1], width, width, logits.shape[1], 1)
    packed = jnp.concatenate(
        [hidden_sum, per_token_b.astype(F32), final, g_logits, losses[:, None]], axis=1
    )
    every = dp.gather(packed).reshape(total_seqs, sum(sizes))
    h_all, g_all, f_all, l_all, loss_all = jnp.split(
        every, [sum(sizes[: i + 1]) for i in range(4)], axis=1
    )
    loss = jnp.sum(loss_all) / total_seqs
    own_d = width // dp.n
    g_own = lax.dynamic_slice_in_dim(g_all, dp.idx * own_d, own_d, axis=1)
    f_own = lax.dynamic_slice_in_dim(f_all, dp.idx * own_d, own_d, axis=1)
    down_weight_gradient = jnp.dot(h_all.T, g_own, precision=lax.Precision.HIGHEST)
    grad_head = jnp.dot(f_own.T, l_all, precision=lax.Precision.HIGHEST)

    n2_all = jnp.concatenate(normed_two, axis=1)
    up_term = mm(n2_all, jnp.concatenate(g_pre, axis=1), "nld,nlf->df").astype(BF16)
    up_weight_gradient = dp.reduce(up_term.reshape(dp.n, own_d, -1))

    g_second_all = jnp.concatenate(g_second, axis=1)
    context_all = jnp.concatenate(context, axis=1)
    out_term = mm(context_all, g_second_all, "nlh,nld->hd").astype(BF16)
    output_weight_gradient = dp.reduce(
        jnp.moveaxis(out_term.reshape(cols, dp.n, own_d), 1, 0)
    )

    g_context = mm(g_second_all, out_w, "nld,hd->nlh")
    delta = (
        (g_context * context_all.astype(F32))
        .reshape(groups, total_len, heads, HEAD_WIDTH)
        .sum(axis=-1)
    )
    g_ctx = g_context.astype(BF16).reshape(groups, total_len, heads, HEAD_WIDTH)
    p_all = jnp.concatenate(probs, axis=2)
    g_vals = mm(p_all, g_ctx, "nhqk,nqhe->nkhe")
    g_probs = mm(g_ctx, vals, "nqhe,nkhe->nhqk")
    g_scores = (
        p_all.astype(F32) * (g_probs - jnp.swapaxes(delta, 1, 2)[..., None]) * scale
    ).astype(BF16)
    g_query = mm(g_scores, keys, "nhqk,nkhe->nqhe")
    g_keys = mm(g_scores, query, "nhqk,nqhe->nkhe")
    g_qkv = jnp.stack([g_query, g_keys, g_vals], axis=2).astype(BF16)
    g_qkv = g_qkv.reshape(groups, total_len, 3 * cols)
    normed_all = jnp.concatenate(normed, axis=1)
    qkv_term = mm(normed_all, g_qkv, "nld,nlc->dc").astype(BF16)
    query_key_value_gradient = dp.reduce(qkv_term.reshape(dp.n, own_d, -1)).reshape(
        own_d, 3, cols
    )
    return (
        loss,
        query_key_value_gradient,
        output_weight_gradient,
        up_weight_gradient,
        down_weight_gradient,
        grad_head,
    )


def solution(mesh):
    placed = (
        P("dp", "tensor"),
        P("dp"),
        P("dp"),
        P("tensor", None),
        P("dp", None, "tensor"),
        P("tensor", "dp"),
        P("dp", "tensor"),
        P("tensor", "dp"),
        P("dp", None),
    )
    return jax.shard_map(
        per_device,
        mesh=mesh,
        in_specs=placed,
        out_specs=(
            P(),
            P("dp", None, "tensor"),
            P("tensor", "dp"),
            P("dp", "tensor"),
            P("tensor", "dp"),
            P("dp", None),
        ),
        check_vma=False,
    )
```

```python
import jax
import jax.numpy as jnp
from jax import lax
from jax.experimental import pallas as pl
from jax.experimental.pallas import tpu as pltpu
from jax.sharding import PartitionSpec as P

HEAD_WIDTH = 64
EPS = 1e-05
GELU_C = 0.7978845608028654
GELU_A = 0.044715


F32 = jnp.float32
BF16 = jnp.bfloat16


def normalize(values):
    mean = jnp.mean(values, axis=-1, keepdims=True)
    centered = values - mean
    return centered * lax.rsqrt(jnp.mean(centered * centered, axis=-1, keepdims=True) + EPS)


def gelu_and_slope(v):
    inner = GELU_C * (v + GELU_A * v * v * v)
    t = jnp.tanh(inner)
    act = 0.5 * v * (1.0 + t)
    slope = 0.5 * (1.0 + t) + 0.5 * v * (1.0 - t * t) * GELU_C * (1.0 + 3.0 * GELU_A * v * v)
    return act, slope


def mm(a, b, spec):
    return jnp.einsum(spec, a, b, preferred_element_type=F32)


class Tensor:
    def __init__(self):
        self.n = lax.axis_size("tensor")
        self.rank = lax.axis_index("tensor")
        self.xor = self.n & (self.n - 1) == 0

    def to(self, r, j):
        return r ^ j if self.xor else (r + j) % self.n

    def send(self, value, j):
        return lax.ppermute(value, "tensor", [(r, self.to(r, j)) for r in range(self.n)])

    def fetch(self, value, j):
        return lax.ppermute(value, "tensor", [(self.to(r, j), r) for r in range(self.n)])

    def gather(self, value):
        return [value] + [self.fetch(value, j) for j in range(1, self.n)]


class Groups:
    def __init__(self):
        self.n = lax.axis_size("dp")
        self.w = 2 if self.n % 2 == 0 else 1
        self.m = self.n // self.w
        idx = lax.axis_index("dp")
        self.idx = idx
        self.z = idx // self.w
        self.c = idx % self.w

    def shift(self, value, k):
        pairs = []
        for z in range(self.m):
            for c in range(self.w):
                pairs.append((((z + k) % self.m) * self.w + c, z * self.w + c))
        return lax.ppermute(value, "dp", pairs)

    def swap(self, value):
        pairs = [(i, i ^ 1) for i in range(self.n)]
        return lax.ppermute(value, "dp", pairs)

    def gather(self, shard):
        ring = jnp.stack([shard] + [self.shift(shard, k) for k in range(1, self.m)], axis=0)
        if self.w == 1:
            return ring
        return jnp.concatenate([ring, self.swap(ring)], axis=0)

    def reduce_pair(self, blocks):
        if self.w == 1:
            return blocks
        keep, away = blocks[: self.m], blocks[self.m :]
        return (keep.astype(F32) + self.swap(away).astype(F32)).astype(BF16)

    def reduce_ring(self, pair):
        total = pair[0].astype(F32)
        for k in range(1, self.m):
            total = total + self.shift(pair[k], self.m - k).astype(F32)
        return total

    def roll(self, x, start, step):
        return lax.dynamic_slice_in_dim(
            jnp.concatenate([x, x], axis=-1), start * step, self.m * step, axis=x.ndim - 1
        )

    def to_relative(self, x):
        step = x.shape[-1] // self.n
        sides = [
            jnp.concatenate(
                [
                    x[..., (z * self.w + c) * step : (z * self.w + c + 1) * step]
                    for z in range(self.m)
                ],
                axis=-1,
            )
            for c in range(self.w)
        ]
        if self.w == 1:
            return self.roll(sides[0], self.z, step)
        mine = jnp.where(self.c == 0, sides[0], sides[1])
        other = jnp.where(self.c == 0, sides[1], sides[0])
        return jnp.concatenate(
            [self.roll(mine, self.z, step), self.roll(other, self.z, step)], axis=-1
        )

    def to_true(self, x):
        step = x.shape[-1] // self.n
        back = (self.m - self.z) % self.m
        if self.w == 1:
            return self.roll(x, back, step)
        half = self.m * step
        mine = self.roll(x[..., :half], back, step)
        other = self.roll(x[..., half:], back, step)
        low = jnp.where(self.c == 0, mine, other)
        high = jnp.where(self.c == 0, other, mine)
        lead = x.shape[:-1]
        both = [low.reshape(lead + (self.m, step)), high.reshape(lead + (self.m, step))]
        return jnp.stack(both, axis=-2).reshape(x.shape)


PAIR = 2 * HEAD_WIDTH
SCALE = HEAD_WIDTH ** (-0.5)
NT = (((1,), (1,)), ((), ()))
NN = (((1,), (0,)), ((), ()))


def dot(a, b, dims):
    return lax.dot_general(a, b, dims, preferred_element_type=F32)


def one_head(pair, i):
    lane = lax.broadcasted_iota(jnp.int32, pair.shape, 1)
    return jnp.where((lane >= HEAD_WIDTH) == (i == 1), pair, jnp.zeros_like(pair))


def attend_kernel(live_ref, q_ref, k_ref, v_ref, o_ref, lse_ref):
    seen = live_ref[0] > 0
    keys = k_ref[0]
    vals_t = v_ref[0].astype(F32).T.astype(BF16)
    outs = []
    for i in range(2):
        scores = dot(keys, one_head(q_ref[0], i), NT) * SCALE
        scores = jnp.where(seen, scores, -1e30)
        top = jnp.max(scores, axis=0, keepdims=True)
        expo = jnp.exp(scores - top)
        total = jnp.sum(expo, axis=0, keepdims=True)
        got = dot(vals_t[i * HEAD_WIDTH : (i + 1) * HEAD_WIDTH], expo.astype(BF16), NN)
        outs.append(got / total)
        lse_ref[0, i] = top + jnp.log(total)
    o_ref[0] = jnp.concatenate(outs, axis=0).T.astype(BF16)


def attend_block(qkv, live_col, j, length):
    groups, total, three = qkv.shape
    cols = three // 3
    pairs = cols // PAIR
    return pl.pallas_call(
        attend_kernel,
        grid=(groups, pairs),
        in_specs=[
            pl.BlockSpec((1, total, 1), lambda g, h: (g, 0, 0)),
            pl.BlockSpec((1, length, PAIR), lambda g, h: (g, j, h)),
            pl.BlockSpec((1, total, PAIR), lambda g, h: (g, 0, pairs + h)),
            pl.BlockSpec((1, total, PAIR), lambda g, h: (g, 0, 2 * pairs + h)),
        ],
        out_specs=[
            pl.BlockSpec((1, length, PAIR), lambda g, h: (g, 0, h)),
            pl.BlockSpec((1, 2, 1, length), lambda g, h: (g, h, 0, 0)),
        ],
        out_shape=[
            jax.ShapeDtypeStruct((groups, length, cols), BF16),
            jax.ShapeDtypeStruct((groups, 2 * pairs, 1, length), F32),
        ],
        name="attend",
    )(live_col, qkv, qkv, qkv)


def attend_back_kernel(
    live_ref, q_ref, k_ref, v_ref, g_ref, o_ref, lse_ref, dq_ref, dk_ref, dv_ref, dk_acc, dv_acc
):
    step = pl.program_id(2)

    @pl.when(step == 0)
    def _():
        dk_acc[...] = jnp.zeros_like(dk_acc)
        dv_acc[...] = jnp.zeros_like(dv_acc)

    seen = live_ref[0] > 0
    keys = k_ref[0]
    vals = v_ref[0]
    keys_t = keys.astype(F32).T.astype(BF16)
    grad = g_ref[0]
    dots_t = (grad.astype(F32) * o_ref[0].astype(F32)).T
    pieces = []
    for i in range(2):
        part = slice(i * HEAD_WIDTH, (i + 1) * HEAD_WIDTH)
        q_i = one_head(q_ref[0], i)
        g_i = one_head(grad, i)
        delta = jnp.sum(dots_t[part], axis=0, keepdims=True)
        scores = jnp.where(seen, dot(keys, q_i, NT) * SCALE, -1e30)
        probs = jnp.exp(scores - lse_ref[0, i])
        g_probs = dot(vals, g_i, NT)
        g_scores = (probs * ((g_probs - delta) * SCALE)).astype(BF16)
        dv_acc[...] += dot(probs.astype(BF16), g_i, NN)
        dk_acc[...] += dot(g_scores, q_i, NN)
        pieces.append(dot(keys_t[part], g_scores, NN))
    dq_ref[0] = jnp.concatenate(pieces, axis=0).T.astype(BF16)

    @pl.when(step == pl.num_programs(2) - 1)
    def _():
        dk_ref[0] = dk_acc[...].astype(BF16)
        dv_ref[0] = dv_acc[...].astype(BF16)


def attend_back(qkv, live_col, grad, out, lse, length):
    groups, total, three = qkv.shape
    cols = three // 3
    pairs = cols // PAIR
    chunk = pl.BlockSpec((1, length, PAIR), lambda g, h, c: (g, c, h))
    whole = pl.BlockSpec((1, total, PAIR), lambda g, h, c: (g, 0, h))
    return pl.pallas_call(
        attend_back_kernel,
        grid=(groups, pairs, total // length),
        in_specs=[
            pl.BlockSpec((1, total, 1), lambda g, h, c: (g, 0, 0)),
            chunk,
            pl.BlockSpec((1, total, PAIR), lambda g, h, c: (g, 0, pairs + h)),
            pl.BlockSpec((1, total, PAIR), lambda g, h, c: (g, 0, 2 * pairs + h)),
            chunk,
            chunk,
            pl.BlockSpec((1, 2, 1, length), lambda g, h, c: (g, h, 0, c)),
        ],
        out_specs=[chunk, whole, whole],
        out_shape=[jax.ShapeDtypeStruct((groups, total, cols), BF16)] * 3,
        scratch_shapes=[pltpu.VMEM((total, PAIR), F32)] * 2,
        name="attend_back",
    )(live_col, qkv, qkv, qkv, grad, out, lse)


def rows_full(blocks):
    return blocks.reshape((blocks.shape[0] * blocks.shape[1],) + blocks.shape[2:])


def cols_full(blocks):
    return jnp.moveaxis(blocks, 0, 1).reshape(blocks.shape[1], -1)


def per_device(
    token_ids,
    lengths,
    teacher_bins,
    embed_table,
    query_key_value_matrix,
    output_matrix,
    up_matrix,
    down_matrix,
    w_head,
):
    tp = Tensor()
    dp = Groups()
    nt = tp.n
    groups, local_len = token_ids.shape
    total_len = local_len * nt
    width = embed_table.shape[1]
    vocab_local = embed_table.shape[0]
    blocks = range(nt)

    hold = lax.optimization_barrier
    ids = jnp.concatenate(tp.gather(token_ids), axis=0)
    qkv_shard = query_key_value_matrix.reshape(query_key_value_matrix.shape[0], -1)
    ids, qkv_shard = hold((ids, qkv_shard))
    shifted = ids - tp.rank * vocab_local
    inside = (shifted >= 0) & (shifted < vocab_local)
    rows = jnp.take(embed_table, jnp.clip(shifted, 0, vocab_local - 1), axis=0)
    rows = jnp.where(inside[..., None], rows, jnp.zeros((), BF16))
    cols_shard = jnp.concatenate([output_matrix, down_matrix], axis=0)
    rows_shard = jnp.concatenate([up_matrix, w_head], axis=1)
    rows, cols_shard, rows_shard = hold((rows, cols_shard, rows_shard))

    order = list(range(1, nt))[::-1]
    arrived = [tp.send(rows[j * groups : (j + 1) * groups], j) for j in order]
    first_f = rows[:groups].astype(F32)
    for piece in arrived:
        first_f = first_f + piece.astype(F32)
    first_f = dp.to_relative(first_f.astype(BF16)).astype(F32)
    first_normed = normalize(first_f).astype(BF16)
    normed = tp.gather(first_normed)

    qkv_w = rows_full(dp.gather(qkv_shard))
    cols_w = cols_full(dp.gather(cols_shard))
    out_w, down_w = cols_w[: output_matrix.shape[0]], cols_w[output_matrix.shape[0] :]
    rows_w = rows_full(dp.gather(rows_shard))
    up_w, head_w = rows_w[:, : up_matrix.shape[1]], rows_w[:, up_matrix.shape[1] :].astype(F32)

    cols = query_key_value_matrix.shape[2]
    qkv = jnp.concatenate(
        [mm(normed[j], qkv_w, "nld,dc->nlc").astype(BF16) for j in blocks], axis=1
    )

    at = [tp.to(tp.rank, j) * local_len + jnp.arange(local_len, dtype=jnp.int32) for j in blocks]
    live = [(at[j][None, :] < lengths[:, None]).astype(F32) for j in blocks]
    live_all = jnp.concatenate(live, axis=1)
    live_col = live_all[:, :, None]

    lse = [None] * nt
    context = [None] * nt
    arrived = []
    for j in order + [0]:
        context[j], lse[j] = attend_block(qkv, live_col, j, local_len)
        part = mm(context[j], out_w, "nlh,hd->nld").astype(BF16)
        if j:
            arrived.append(tp.send(part, j))
        else:
            attn_sum = part.astype(F32)
    for piece in arrived:
        attn_sum = attn_sum + piece.astype(F32)
    second = (first_f + attn_sum).astype(BF16)
    second_f = second.astype(F32)
    normed_two_f, norm_back = jax.vjp(normalize, second_f)
    normed_two = tp.gather(normed_two_f.astype(BF16))

    slopes = []
    hidden_sum = 0.0
    for j in blocks:
        act, slope = gelu_and_slope(mm(normed_two[j], up_w, "nld,df->nlf"))
        slopes.append((slope * live[j][:, :, None]).astype(BF16))
        hidden_sum = hidden_sum + jnp.sum(
            act.astype(BF16).astype(F32) * live[j][:, :, None], axis=1
        )
    coarse = hidden_sum.astype(BF16)
    fine = (hidden_sum - coarse.astype(F32)).astype(BF16)
    pooled_part = mm(jnp.stack([coarse, fine]), down_w, "knf,fd->knd").sum(axis=0)
    pooled_part = pooled_part + jnp.sum(second_f * live[0][:, :, None], axis=1)
    counts = lengths.astype(F32)[:, None]
    pooled_sum = pooled_part
    for piece in tp.gather(pooled_part)[1:]:
        pooled_sum = pooled_sum + piece
    pooled = pooled_sum / counts
    final, final_back = jax.vjp(normalize, pooled)
    logits = jnp.dot(final, head_w, precision=lax.Precision.HIGHEST)
    top = jnp.max(logits, axis=-1, keepdims=True)
    total_exp = jnp.log(jnp.sum(jnp.exp(logits - top), axis=-1, keepdims=True)) + top
    labels = (
        teacher_bins[:, None] == jnp.arange(logits.shape[1], dtype=jnp.int32)[None, :]
    ).astype(F32)
    losses = total_exp[:, 0] - jnp.sum(logits * labels, axis=-1)
    total_seqs = groups * dp.n
    g_logits = (jnp.exp(logits - total_exp) - labels) / total_seqs
    g_final = jnp.dot(g_logits, head_w.T, precision=lax.Precision.HIGHEST)
    g_pooled = final_back(g_final)[0]
    per_token = g_pooled / counts
    per_token_b = per_token.astype(BF16)

    hidden_g = mm(per_token_b, down_w, "nd,fd->nf")
    g_pre = [(slopes[j].astype(F32) * hidden_g[:, None, :]).astype(BF16) for j in blocks]
    arrived = []
    for j in order:
        part = mm(g_pre[j], up_w, "nlf,df->nld").astype(BF16)
        arrived.append(tp.send(part, j))
    n2_all = jnp.concatenate(normed_two, axis=1)
    own_d = width // dp.n
    up_term = mm(n2_all, jnp.concatenate(g_pre, axis=1), "nld,nlf->df").astype(BF16)
    up_pair = dp.reduce_pair(up_term.reshape(dp.n, own_d, -1))
    g_normed_two = mm(g_pre[0], up_w, "nlf,df->nld").astype(BF16).astype(F32)
    arrived[-1], up_pair = hold((arrived[-1], up_pair))
    for piece in arrived:
        g_normed_two = g_normed_two + piece.astype(F32)
    g_third = per_token[:, None, :] * live[0][:, :, None]
    g_second = tp.gather((g_third + norm_back(g_normed_two)[0]).astype(BF16))
    up_weight_gradient = dp.reduce_ring(up_pair)

    sizes = (hidden_sum.shape[1], width, width, logits.shape[1], 1)
    packed = jnp.concatenate(
        [
            hidden_sum,
            dp.to_true(per_token_b.astype(F32)),
            dp.to_true(final),
            g_logits,
            losses[:, None],
        ],
        axis=1,
    )
    every = dp.gather(packed).reshape(total_seqs, sum(sizes))
    h_all, g_all, f_all, l_all, loss_all = jnp.split(
        every, [sum(sizes[: i + 1]) for i in range(4)], axis=1
    )
    loss = jnp.sum(loss_all) / total_seqs
    g_own = lax.dynamic_slice_in_dim(g_all, dp.idx * own_d, own_d, axis=1)
    f_own = lax.dynamic_slice_in_dim(f_all, dp.idx * own_d, own_d, axis=1)
    down_weight_gradient = jnp.dot(h_all.T, g_own, precision=lax.Precision.HIGHEST)
    grad_head = jnp.dot(f_own.T, l_all, precision=lax.Precision.HIGHEST)

    g_second_all = jnp.concatenate(g_second, axis=1)
    context_all = jnp.concatenate(context, axis=1)
    out_term = mm(context_all, g_second_all, "nlh,nld->hd").astype(BF16)
    out_pair = dp.reduce_pair(jnp.moveaxis(out_term.reshape(cols, dp.n, own_d), 1, 0))
    g_context = jnp.concatenate(
        [mm(g_second[j], out_w, "nld,hd->nlh").astype(BF16) for j in blocks], axis=1
    )
    g_context, out_pair = hold((g_context, out_pair))
    output_weight_gradient = dp.reduce_ring(out_pair)
    g_qkv = jnp.concatenate(
        attend_back(
            qkv, live_col, g_context, context_all, jnp.concatenate(lse, axis=3), local_len
        ),
        axis=2,
    )
    normed_all = jnp.concatenate(normed, axis=1)
    g_qkv, up_weight_gradient, output_weight_gradient = hold(
        (g_qkv, up_weight_gradient, output_weight_gradient)
    )
    qkv_term = mm(normed_all, g_qkv, "nld,nlc->dc").astype(BF16)
    query_key_value_gradient = dp.reduce_ring(
        dp.reduce_pair(qkv_term.reshape(dp.n, own_d, -1))
    ).reshape(own_d, 3, cols)
    return (
        loss,
        query_key_value_gradient,
        output_weight_gradient,
        up_weight_gradient,
        down_weight_gradient,
        grad_head,
    )


def solution(mesh):
    placed = (
        P("dp", "tensor"),
        P("dp"),
        P("dp"),
        P("tensor", None),
        P("dp", None, "tensor"),
        P("tensor", "dp"),
        P("dp", "tensor"),
        P("tensor", "dp"),
        P("dp", None),
    )
    return jax.shard_map(
        per_device,
        mesh=mesh,
        in_specs=placed,
        out_specs=(
            P(),
            P("dp", None, "tensor"),
            P("tensor", "dp"),
            P("dp", "tensor"),
            P("tensor", "dp"),
            P("dp", None),
        ),
        check_vma=False,
    )
```
